32 devices in a mesh: aa: 4 (over z), ba: 2 (over y), col: 4 (over x, core).
Axes of the slice: x: 2, y: 2, z: 4, core: 2. Of those that a mesh axis runs over, the one named last changes fastest.
Arguments:
- tokens: bfloat16 [2048, 7168], P(('aa', 'col'), 'ba'), may hold values from -6 to 6
- routing: int32 [2048, 8], P(('aa', 'col')), may hold values from 0 to 15, all different within a row; in each aligned block of 128 rows (0 to 127, 128 to 255, ...) at most 80 rows name the same one
- gate_codes: int32 [2048, 8], P(('aa', 'col')), may hold values from 1 to 65535
- w_gate: bfloat16 [16, 7168, 2048], P(('aa', 'col'), None, 'ba'), may hold values from -0.0625 to 0.0625
- w_up: bfloat16 [16, 7168, 2048], P(('aa', 'col'), None, 'ba'), may hold values from -0.0625 to 0.0625
- w_down: bfloat16 [16, 2048, 7168], P(('aa', 'col'), 'ba'), may hold values from -0.125 to 0.125
Outputs:
- mixed: bfloat16 [2048, 7168], P(('aa', 'col'), 'ba')
The draws below stay inside these ranges and needn't reach their ends.
Inputs may be any that keep to these rules, and one draw needn't show every extreme that they name: `routing`: within each token group of 128 rows (aligned blocks of the rows), no expert is named more than 80 times, a bound that some block reaches. A token names 8 different experts.
All inputs are finite; a program needn't handle non-finite values.
Results may differ from the reference program's by a relative error of at most 0.014.
Values may be sent and summed in bfloat16 or wider, within the bound.
No kernel may reach another device: no remote copies, remote signals or barrier semaphores. Data moves between devices by JAX's collectives and lax.ppermute only.
A program may use at most 192 MiB of HBM per device.

```python
import math
import jax
import jax.numpy as jnp
import numpy as np
from jax import lax

D = 7168
FF = 2048
TOP = 8
TOK_DEV = 128
EXPERTS = 16
TOKENS = 2048
CAP = 80
N_AA = 4
N_BA = 2
N_COL = 4


def touch_ends(entries, stream_key, low, top_value):
    extent = entries.shape
    place = [jax.random.randint(jax.random.fold_in(stream_key, axis), (), 0, extent[axis]) for axis in range(len(extent))]
    entries = entries.at[tuple(place)].set(low)
    longest = extent.index(max(extent))
    place[longest] = (place[longest] + 1) % extent[longest]
    return entries.at[tuple(place)].set(top_value)


def shard_levels(own_key, extent, pieces, least, high):
    loudness = 1.0
    for position, shards_of in pieces:
        heights = jax.random.uniform(jax.random.fold_in(jax.random.fold_in(own_key, 6), position), (shards_of,), jnp.float32, least / len(pieces), high / len(pieces))
        loudness = loudness * jnp.repeat(jnp.exp(heights), extent[position] // shards_of).reshape((-1,) + (1,) * (len(extent) - 1 - position))
    return loudness


def shared_out(own_key, own, number, rows, amount, top, bound, lean):
    order = jax.random.permutation(own_key, amount)
    crowded, usual = shares(amount, rows * top, bound, lean, True), shares(amount, rows * top, bound, lean, False)
    places = jnp.arange(amount)

    def named(sizes, turn):
        used = int((sizes > 0).sum())
        fixed = max(1, used // 4)
        shifted = fixed + (places - fixed + turn * (used - fixed)) % max(1, amount - fixed)
        return jnp.zeros((amount,), jnp.int32).at[order[jnp.where(places < fixed, places, shifted)]].set(jnp.asarray(sizes, jnp.int32))

    sizes = jnp.where(number % 4 == 0, named(crowded, number // 4), named(usual, number - number // 4 - 1))
    mixed = jax.random.permutation(jax.random.fold_in(own, 3), amount)
    giver, taker = mixed[0:amount // 2 * 2:2], mixed[1:amount // 2 * 2:2]
    margin = jnp.minimum(sizes[giver] - 1, bound - sizes[taker]) // 2
    margin = jnp.where((giver == order[0]) | (taker == order[0]) | (sizes[taker] == 0), 0, jnp.maximum(margin, 0))
    shifted = jax.random.randint(jax.random.fold_in(own, 4), (amount // 2,), 0, 1 << 20) % (margin + 1)
    sizes = sizes.at[giver].add(-shifted).at[taker].add(shifted)
    items = jnp.searchsorted(jnp.cumsum(sizes), jnp.arange(rows * top), side="right").astype(jnp.int32)
    listing = items.reshape(top, rows).T
    listing = listing[jax.random.permutation(jax.random.fold_in(own, 1), rows)]
    turn = jax.random.randint(jax.random.fold_in(own, 2), (rows, 1), 0, top)
    return jnp.take_along_axis(listing, (jnp.arange(top)[None, :] + turn) % top, axis=1)


def shares(amount, total, reach, skew, full):
    loads = [(1 << 20) // math.isqrt(grade ** skew) + 1 for grade in range(1, amount + 1)]
    largest = reach if full else min(reach, max(-(-total // amount), total * loads[0] // sum(loads)))
    least = 1 if total - largest >= amount - 1 else 0
    holding, spare = [largest] + [least] * (amount - 1), total - largest - least * (amount - 1)
    while spare > 0:
        free = [i for i in range(1, amount) if holding[i] < largest] or [i for i in range(1, amount) if holding[i] < reach]
        mass, budget = sum([loads[i] for i in free]), spare
        for i in free:
            more = min(reach - holding[i], max(1, budget * loads[i] // mass), spare)
            holding[i] = holding[i] + more
            spare = spare - more
    return np.array(holding)


def noise(stream_key, dims, spread, bound, shards=(), held_as=jnp.bfloat16):
    array = jax.random.normal(stream_key, dims, jnp.float32) * spread
    if len(shards) > 0:
        array = shard_levels(stream_key, dims, shards, -0.22, 0.18) * array
    return jnp.clip(array, min=-bound, max=bound).astype(held_as)


def setup_inputs(seed: int = 0) -> dict:
    key_of = jax.random.split(jax.random.key(seed), 7)
    tokens = noise(key_of[0], (TOKENS, D), 1.0, 6.0, ((0, 16), (1, 2)))
    routing_keys = jax.random.split(jax.random.fold_in(key_of[1], 1), TOKENS // TOK_DEV)
    routing_turns = jax.random.permutation(jax.random.fold_in(key_of[1], 3), TOKENS // TOK_DEV)
    routing = jax.vmap(lambda own, number: shared_out(jax.random.fold_in(key_of[1], 2), own, number, TOK_DEV, EXPERTS, TOP, CAP, 2))(routing_keys, routing_turns).reshape((TOKENS, TOP))
    gate_codes = touch_ends(jax.random.randint(key_of[2], (TOKENS, TOP), 1, 65536), jax.random.fold_in(key_of[2], 1), 1, 65535).astype(jnp.int32)
    w_gate = noise(key_of[3], (EXPERTS, D, FF), D ** -0.5, 0.0625, ((0, 16), (2, 2)))
    w_up = noise(key_of[4], (EXPERTS, D, FF), D ** -0.5, 0.0625, ((0, 16), (2, 2)))
    w_down = noise(key_of[5], (EXPERTS, FF, D), FF ** -0.5, 0.125, ((0, 16), (1, 2)))
    return {"tokens": tokens, "routing": routing, "gate_codes": gate_codes, "w_gate": w_gate, "w_up": w_up, "w_down": w_down}


route_scale = 2.827


def slot_tables(group_routes):
    flat = group_routes.reshape(-1)
    onehot = (flat[:, None] == jnp.arange(EXPERTS, dtype=jnp.int32)[None, :]).astype(jnp.int32)
    before = jnp.cumsum(onehot, axis=0) - onehot
    pos = jnp.sum(before * onehot, axis=1).astype(jnp.int32)
    slot = (flat * CAP + pos).astype(jnp.int32)
    matched = slot[:, None] == jnp.arange(EXPERTS * CAP, dtype=jnp.int32)[None, :]
    owner = (jnp.arange(flat.shape[0], dtype=jnp.int32) // TOP).astype(jnp.int32)
    slot_token = jnp.sum(jnp.where(matched, owner[:, None], 0), axis=0).astype(jnp.int32)
    live = jnp.any(matched, axis=0)
    return slot, slot_token.reshape(EXPERTS, CAP), live.reshape(EXPERTS, CAP)


def reference(tokens, routing, gate_codes, w_gate, w_up, w_down):
    groups = N_AA * N_COL
    slot, slot_token, live = jax.vmap(slot_tables)(routing.reshape(groups, TOK_DEV, TOP))
    grouped = tokens.reshape(groups, TOK_DEV, D)
    width = FF // N_BA
    group_ids = jnp.arange(groups, dtype=jnp.int32)[:, None]

    def expert(packed):
        wg, wu, wd, index, alive = packed
        rows = grouped[group_ids, index]
        rows = jnp.where(alive[:, :, None], rows, jnp.zeros((), jnp.bfloat16)).reshape(groups * CAP, D)
        total = jnp.zeros((groups * CAP, D), jnp.float32)
        for part in range(N_BA):
            gate = jnp.dot(rows, wg[:, part * width:(part + 1) * width], preferred_element_type=jnp.float32)
            upper = jnp.dot(rows, wu[:, part * width:(part + 1) * width], preferred_element_type=jnp.float32)
            hidden = (jax.nn.silu(gate) * upper).astype(jnp.bfloat16)
            piece = jnp.dot(hidden, wd[part * width:(part + 1) * width, :], preferred_element_type=jnp.float32)
            piece = lax.optimization_barrier(piece.astype(jnp.bfloat16))
            total = total + piece.astype(jnp.float32)
        return total.astype(jnp.bfloat16).reshape(groups, CAP, D)

    outputs = lax.map(expert, (w_gate, w_up, w_down, jnp.transpose(slot_token, (1, 0, 2)), jnp.transpose(live, (1, 0, 2))))
    outputs = jnp.transpose(outputs, (1, 0, 2, 3)).reshape(groups, EXPERTS * CAP, D)
    codes = gate_codes.astype(jnp.float32)
    weight = route_scale * codes / jnp.sum(codes, axis=1, keepdims=True)
    weight = weight.reshape(groups, TOK_DEV, TOP)

    def combine(packed):
        table, slots, scores = packed
        picked = table[slots].reshape(TOK_DEV, TOP, D).astype(jnp.float32)
        return jnp.einsum("tk,tkd->td", scores, picked).astype(jnp.bfloat16)

    mixed = lax.map(combine, (outputs, slot, weight))
    return mixed.reshape(TOKENS, D)
```

```python
import jax
import jax.numpy as jnp
from jax import lax
from jax.sharding import PartitionSpec as P

route_scale = 2.827
n_chunks = 4


def shift(value, axis, inner, outer_n, inner_n, step):
    pairs = []
    for out in range(outer_n):
        for low in range(inner_n):
            if inner:
                to = out * inner_n + (low + step) % inner_n
            else:
                to = (out + step) % outer_n * inner_n + low
            pairs.append((out * inner_n + low, to))
    return lax.ppermute(value, axis, pairs)


class Phase:
    def __init__(self, axis, inner, outer_n, inner_n):
        self.args = (axis, inner, outer_n, inner_n)
        self.n = inner_n if inner else outer_n

    def gather(self, value):
        return [value] + [shift(value, *self.args, s) for s in range(1, self.n)]

    def reduce(self, blocks):
        arrived = [shift(blocks[s], *self.args, self.n - s) for s in range(1, self.n)]
        total = blocks[0].astype(jnp.float32)
        for block in arrived:
            total = total + block.astype(jnp.float32)
        return total.astype(jnp.bfloat16)


def on_device(tokens, routing, gate_codes, w_gate, w_up, w_down):
    n_aa = lax.axis_size("aa")
    n_ba = lax.axis_size("ba")
    n_col = lax.axis_size("col")
    experts = n_aa * n_col
    inner_n = 2 if n_col % 2 == 0 else 1
    zed = Phase("aa", False, n_aa, 1)
    wide = Phase("col", False, n_col // inner_n, inner_n)
    pair = Phase("col", True, n_col // inner_n, inner_n)
    feat = Phase("ba", False, n_ba, 1)
    mine = lax.axis_index("aa") * n_col + lax.axis_index("col")
    half = lax.axis_index("ba")
    tok_rows, width = tokens.shape
    rows = tok_rows // n_chunks

    codes = gate_codes.astype(jnp.float32)
    weight = route_scale * codes / jnp.sum(codes, axis=1, keepdims=True)
    named = routing[None, :, :] == jnp.arange(experts, dtype=jnp.int32)[:, None, None]
    scores = jnp.sum(jnp.where(named, weight[None, :, :], 0.0), axis=2)
    scores = jnp.stack(zed.gather(scores))
    scores = jnp.stack(wide.gather(scores))
    scores = jnp.stack(pair.gather(scores))
    own = jnp.arange(experts, dtype=jnp.int32)[:, None] == mine
    scores = jnp.sum(jnp.where(own, scores, 0.0), axis=3)

    gate_local = w_gate[0]
    up_local = w_up[0]
    down_local = w_down[0]

    def fetch(piece, number):
        value = jnp.stack(zed.gather(piece))
        if number % 2 == 0:
            value = jnp.stack(wide.gather(value))
            parts = feat.gather(value)
        else:
            sides = feat.gather(value)
            parts = [jnp.stack(wide.gather(v)) for v in sides]
        parts = [jnp.stack(pair.gather(v)) for v in parts]
        flat = [v.reshape(-1, width) for v in parts]
        ordered = []
        for b in range(n_ba):
            pick = flat[0]
            for s in range(1, n_ba):
                pick = jnp.where((half - s) % n_ba == b, flat[s], pick)
            ordered.append(pick)
        return jnp.concatenate(ordered, axis=1)

    def expert(x, number):
        gate = jnp.dot(x, gate_local, preferred_element_type=jnp.float32)
        upper = jnp.dot(x, up_local, preferred_element_type=jnp.float32)
        hidden = (jax.nn.silu(gate) * upper).astype(jnp.bfloat16)
        scale = lax.slice_in_dim(scores, number * rows, (number + 1) * rows, axis=3).reshape(-1, 1)
        out = jnp.dot(hidden, down_local, preferred_element_type=jnp.float32)
        return (out * scale).astype(jnp.bfloat16)

    def give_back(out, number):
        value = out.reshape(pair.n, wide.n, zed.n, rows, n_ba * width)
        value = pair.reduce([value[s] for s in range(pair.n)])
        sides = [
            lax.dynamic_slice_in_dim(value, (half - s) % n_ba * width, width, axis=3)
            for s in range(n_ba)
        ]
        if number % 2 == 0:
            value = feat.reduce(sides)
            value = wide.reduce([value[s] for s in range(wide.n)])
        else:
            sides = [wide.reduce([v[s] for s in range(wide.n)]) for v in sides]
            value = feat.reduce(sides)
        return zed.reduce([value[s] for s in range(zed.n)])

    xs = [fetch(lax.slice_in_dim(tokens, c * rows, (c + 1) * rows, axis=0), c) for c in range(n_chunks)]
    outs = [expert(xs[c], c) for c in range(n_chunks)]
    return jnp.concatenate([give_back(outs[c], c) for c in range(n_chunks)], axis=0)


def solution(mesh):
    return jax.shard_map(
        on_device,
        mesh=mesh,
        in_specs=(
            P(("aa", "col"), "ba"),
            P(("aa", "col"), None),
            P(("aa", "col"), None),
            P(("aa", "col"), None, "ba"),
            P(("aa", "col"), None, "ba"),
            P(("aa", "col"), "ba", None),
        ),
        out_specs=P(("aa", "col"), "ba"),
        check_vma=False,
    )
```

```python
import functools

import jax
import jax.numpy as jnp
from jax import lax
from jax.experimental import pallas as pl
from jax.experimental.pallas import tpu as pltpu
from jax.sharding import PartitionSpec as P


route_scale = 2.827
n_gathers = 2
n_calls = 4


class Phase:
    def __init__(self, axis, inner, outer_n, inner_n):
        self.axis, self.inner, self.outer_n, self.inner_n = axis, inner, outer_n, inner_n
        self.n = inner_n if inner else outer_n
        place = lax.axis_index(axis)
        self.me = place % inner_n if inner else place // inner_n

    def shift(self, value, step):
        pairs = []
        for out in range(self.outer_n):
            for low in range(self.inner_n):
                if self.inner:
                    to = out * self.inner_n + (low + step) % self.inner_n
                else:
                    to = (out + step) % self.outer_n * self.inner_n + low
                pairs.append((out * self.inner_n + low, to))
        return lax.ppermute(value, self.axis, pairs)

    def gather(self, value):
        return jnp.stack([value] + [self.shift(value, s) for s in range(1, self.n)])

    def ordered(self, value, axis):
        return jnp.take(value, (self.me - jnp.arange(self.n)) % self.n, axis=axis)

    def blocks(self, value, axis, moving):
        if not moving:
            return [lax.index_in_dim(value, s, axis, keepdims=False) for s in range(self.n)]
        return [
            lax.dynamic_index_in_dim(value, (self.me - s) % self.n, axis, keepdims=False)
            for s in range(self.n)
        ]

    def send(self, blocks):
        return [self.shift(blocks[s], self.n - s) for s in range(1, self.n)]


def total_of(own, arrived):
    total = own.astype(jnp.float32)
    for block in arrived:
        total = total + block.astype(jnp.float32)
    return total.astype(jnp.bfloat16)


def hidden_body(steps, place, *refs):
    n_x = len(refs) - 5
    xs = refs[:n_x]
    wg, wu, out, gate, upper = refs[n_x:]
    k = pl.program_id(0)
    x = jnp.concatenate([r[...].reshape(-1, r.shape[-1]) for r in xs], axis=0)
    g = jnp.dot(x, wg[0], preferred_element_type=jnp.float32)
    u = jnp.dot(x, wu[0], preferred_element_type=jnp.float32)

    @pl.when(k == 0)
    def _():
        gate[...] = g
        upper[...] = u

    @pl.when(k > 0)
    def _():
        gate[...] += g
        upper[...] += u

    @pl.when(k == steps - 1)
    def _():
        v = gate[...]
        out[...] = (v / (1.0 + jnp.exp(-v)) * upper[...]).astype(jnp.bfloat16)


def down_body(place, hidden, wd, scale, *outs):
    y = jnp.dot(hidden[...], wd[0], preferred_element_type=jnp.float32)
    y = (y * scale[...]).astype(jnp.bfloat16)
    each = y.shape[0] // len(outs)
    for s, out in enumerate(outs):
        out[0] = y[s * each : (s + 1) * each]


def on_device(tokens, routing, gate_codes, w_gate, w_up, w_down):
    n_aa = lax.axis_size("aa")
    n_ba = lax.axis_size("ba")
    n_col = lax.axis_size("col")
    experts = n_aa * n_col
    n_low = 2 if n_col % 2 == 0 else 1
    n_high = n_col // n_low
    zed = Phase("aa", False, n_aa, 1)
    wide = Phase("col", False, n_high, n_low)
    pair = Phase("col", True, n_high, n_low)
    feat = Phase("ba", False, n_ba, 1)
    mine = lax.axis_index("aa") * n_col + lax.axis_index("col")
    tok_rows, width = tokens.shape
    hidden_n = w_gate.shape[2]
    rows = tok_rows // n_calls
    each = n_aa * n_high * rows
    tall = n_low * each
    block = 896 if width % 896 == 0 else width
    per = width // block
    steps = n_ba * per
    place = jnp.stack([feat.me, pair.me]).astype(jnp.int32)

    codes = gate_codes.astype(jnp.float32)
    weight = route_scale * codes / jnp.sum(codes, axis=1, keepdims=True)
    named = routing[None, :, :] == jnp.arange(experts, dtype=jnp.int32)[:, None, None]
    scores = jnp.sum(jnp.where(named, weight[None, :, :], 0.0), axis=2)
    scores = wide.gather(zed.gather(scores))
    scores = pair.gather(scores)
    own = jnp.arange(experts, dtype=jnp.int32)[:, None] == mine
    scores = jnp.sum(jnp.where(own, scores, 0.0), axis=3)
    scores = wide.ordered(zed.ordered(scores, 2), 1)
    scores = jnp.swapaxes(scores, 1, 2)

    def source(k, place):
        return (place[0] + n_ba - k // per) % n_ba

    def hidden_of(gathered, number):
        specs = [
            pl.BlockSpec(
                (n_aa, 1, n_high, 1, rows, block),
                functools.partial(
                    lambda s, k, place: (0, source(k, place), 0, (place[1] + n_low - s) % n_low, number, k % per), s
                ),
            )
            for s in range(n_low)
        ]
        weights = pl.BlockSpec((1, block, hidden_n), lambda k, place: (0, source(k, place) * per + k % per, 0))
        return pl.pallas_call(
            functools.partial(hidden_body, steps),
            grid_spec=pltpu.PrefetchScalarGridSpec(
                num_scalar_prefetch=1,
                grid=(steps,),
                in_specs=specs + [weights, weights],
                out_specs=pl.BlockSpec((tall, hidden_n), lambda k, place: (0, 0)),
                scratch_shapes=[pltpu.VMEM((tall, hidden_n), jnp.float32)] * 2,
            ),
            out_shape=jax.ShapeDtypeStruct((tall, hidden_n), jnp.bfloat16),
            cost_estimate=pl.CostEstimate(
                flops=4 * tall * n_ba * width * hidden_n,
                transcendentals=tall * hidden_n,
                bytes_accessed=4 * n_ba * width * hidden_n + 2 * tall * n_ba * width,
            ),
            compiler_params=pltpu.CompilerParams(vmem_limit_bytes=48 * 1024 * 1024),
        )(place, *[gathered] * n_low, w_gate, w_up)

    def out_of(hidden, number):
        scale = lax.slice_in_dim(scores, number * rows, (number + 1) * rows, axis=3).reshape(-1, 1)
        return pl.pallas_call(
            down_body,
            grid_spec=pltpu.PrefetchScalarGridSpec(
                num_scalar_prefetch=1,
                grid=(steps,),
                in_specs=[
                    pl.BlockSpec((tall, hidden_n), lambda k, place: (0, 0)),
                    pl.BlockSpec((1, hidden_n, block), lambda k, place: (0, 0, source(k, place) * per + k % per)),
                    pl.BlockSpec((tall, 1), lambda k, place: (0, 0)),
                ],
                out_specs=[pl.BlockSpec((1, each, block), lambda k, place: (k // per, 0, k % per))] * n_low,
            ),
            out_shape=[jax.ShapeDtypeStruct((n_ba, each, width), jnp.bfloat16)] * n_low,
            cost_estimate=pl.CostEstimate(
                flops=2 * tall * n_ba * width * hidden_n,
                transcendentals=0,
                bytes_accessed=2 * n_ba * width * hidden_n + 2 * tall * n_ba * width,
            ),
            compiler_params=pltpu.CompilerParams(vmem_limit_bytes=48 * 1024 * 1024),
        )(place, hidden, w_down, scale)

    def give_back(outs):
        arrived = pair.send(outs)
        yield []
        value = total_of(outs[0], arrived).reshape(n_ba, n_aa, n_high, rows, width)
        middle = width // 256 * 128
        first, second = value[..., :middle], value[..., middle:]
        sides = feat.blocks(first, 0, False)
        walls = wide.blocks(second, 2, True)
        got_a, got_b = feat.send(sides), wide.send(walls)
        yield [value]
        first = total_of(sides[0], got_a)
        second = total_of(walls[0], got_b)
        walls = wide.blocks(first, 1, True)
        sides = feat.blocks(second, 0, False)
        got_a, got_b = wide.send(walls), feat.send(sides)
        yield [first, second]
        value = jnp.concatenate([total_of(walls[0], got_a), total_of(sides[0], got_b)], axis=-1)
        floors = zed.blocks(value, 0, True)
        arrived = zed.send(floors)
        yield [value]
        yield [total_of(floors[0], arrived)]

    each_gather = tok_rows // n_gathers
    gathered = []
    for c in range(n_gathers):
        piece = lax.slice_in_dim(tokens, c * each_gather, (c + 1) * each_gather, axis=0)
        piece = lax.all_gather(piece, ("aa", "ba", "col"), axis=0, tiled=False)
        gathered.append(piece.reshape(n_aa, n_ba, n_high, n_low, each_gather, width))

    def tie(value, others):
        return lax.optimization_barrier((value, *others))[0] if others else value

    per_gather = n_calls // n_gathers
    sums, last = [], {}

    def step(number):
        last[number] = next(sums[number])
        return last[number]

    plan = [((), ()), ((), (0,)), ((1, 0, 1, 0, 1), ()), ((), (2, 0, 1))]
    outs = []
    for number in range(n_calls):
        before, between = plan[number]
        ready = [v for c in before for v in step(c)]
        hidden = hidden_of(tie(gathered[number // per_gather], ready + outs), number % per_gather)
        ready = [v for c in between for v in step(c)]
        outs = list(out_of(tie(hidden, ready), number))
        sums.append(give_back(outs))
        step(number)
    for number in range(n_calls):
        for last[number] in sums[number]:
            pass
    return jnp.concatenate([last[c][0] for c in range(n_calls)], axis=0)


def solution(mesh):
    return jax.shard_map(
        on_device,
        mesh=mesh,
        in_specs=(
            P(("aa", "col"), "ba"),
            P(("aa", "col"), None),
            P(("aa", "col"), None),
            P(("aa", "col"), None, "ba"),
            P(("aa", "col"), None, "ba"),
            P(("aa", "col"), "ba", None),
        ),
        out_specs=P(("aa", "col"), "ba"),
        check_vma=False,
    )
```

```python
import functools

import jax
import jax.numpy as jnp
from jax import lax
from jax.experimental import pallas as pl
from jax.experimental.pallas import tpu as pltpu
from jax.sharding import PartitionSpec as P


route_scale = 2.827
n_calls = 4
n_walked = 2


class Phase:
    def __init__(self, axis, inner, outer_n, inner_n):
        self.axis, self.inner, self.outer_n, self.inner_n = axis, inner, outer_n, inner_n
        self.n = inner_n if inner else outer_n
        place = lax.axis_index(axis)
        self.me = place % inner_n if inner else place // inner_n

    def shift(self, value, step):
        pairs = []
        for out in range(self.outer_n):
            for low in range(self.inner_n):
                if self.inner:
                    to = out * self.inner_n + (low + step) % self.inner_n
                else:
                    to = (out + step) % self.outer_n * self.inner_n + low
                pairs.append((out * self.inner_n + low, to))
        return lax.ppermute(value, self.axis, pairs)

    def gather(self, value, axis=0):
        return jnp.stack([value] + [self.shift(value, s) for s in range(1, self.n)], axis=axis)

    def ordered(self, value, axis):
        return jnp.take(value, (self.me - jnp.arange(self.n)) % self.n, axis=axis)

    def blocks(self, value, axis, moving):
        if not moving:
            return [lax.index_in_dim(value, s, axis, keepdims=False) for s in range(self.n)]
        return [
            lax.dynamic_index_in_dim(value, (self.me - s) % self.n, axis, keepdims=False)
            for s in range(self.n)
        ]

    def send(self, blocks):
        return [self.shift(blocks[s], self.n - s) for s in range(1, self.n)]


def total_of(own, arrived):
    total = own.astype(jnp.float32)
    for block in arrived:
        total = total + block.astype(jnp.float32)
    return total.astype(jnp.bfloat16)


def hidden_body(steps, place, *refs):
    n_x = len(refs) - 5
    xs = refs[:n_x]
    wg, wu, out, gate, upper = refs[n_x:]
    k = pl.program_id(0)
    x = jnp.concatenate([r[...].reshape(-1, r.shape[-1]) for r in xs], axis=0)
    g = jnp.dot(x, wg[0], preferred_element_type=jnp.float32)
    u = jnp.dot(x, wu[0], preferred_element_type=jnp.float32)

    @pl.when(k == 0)
    def _():
        gate[...] = g
        upper[...] = u

    @pl.when(k > 0)
    def _():
        gate[...] += g
        upper[...] += u

    @pl.when(k == steps - 1)
    def _():
        v = gate[...]
        out[...] = (v / (1.0 + jnp.exp(-v)) * upper[...]).astype(jnp.bfloat16)


def down_body(place, hidden, wd, scale, *outs):
    y = jnp.dot(hidden[...], wd[0], preferred_element_type=jnp.float32)
    y = (y * scale[...]).astype(jnp.bfloat16)
    each = y.shape[0] // len(outs)
    for s, out in enumerate(outs):
        out[0] = y[s * each : (s + 1) * each]


def on_device(tokens, routing, gate_codes, w_gate, w_up, w_down):
    n_aa = lax.axis_size("aa")
    n_ba = lax.axis_size("ba")
    n_col = lax.axis_size("col")
    experts = n_aa * n_col
    n_low = 2 if n_col % 2 == 0 else 1
    n_high = n_col // n_low
    zed = Phase("aa", False, n_aa, 1)
    wide = Phase("col", False, n_high, n_low)
    pair = Phase("col", True, n_high, n_low)
    feat = Phase("ba", False, n_ba, 1)
    mine = lax.axis_index("aa") * n_col + lax.axis_index("col")
    tok_rows, width = tokens.shape
    hidden_n = w_gate.shape[2]
    rows = tok_rows // n_calls
    each = n_aa * n_high * rows
    tall = n_low * each
    block = 1792 if width % 1792 == 0 else width
    per = width // block
    steps = n_ba * per
    place = jnp.stack([feat.me, pair.me]).astype(jnp.int32)

    codes = gate_codes.astype(jnp.float32)
    weight = route_scale * codes / jnp.sum(codes, axis=1, keepdims=True)
    named = routing[None, :, :] == jnp.arange(experts, dtype=jnp.int32)[:, None, None]
    scores = jnp.sum(jnp.where(named, weight[None, :, :], 0.0), axis=2)
    scores = wide.gather(zed.gather(scores))
    scores = pair.gather(scores)
    own = jnp.arange(experts, dtype=jnp.int32)[:, None] == mine
    scores = jnp.sum(jnp.where(own, scores, 0.0), axis=3)
    walked_scores = jnp.swapaxes(scores, 1, 2)
    scores = wide.ordered(zed.ordered(walked_scores, 1), 2)

    def source(k, place):
        return (place[0] + n_ba - k // per) % n_ba

    def hidden_of(arrays, number):
        if len(arrays) == 1:
            arrays = arrays * n_low
            specs = [
                pl.BlockSpec(
                    (n_aa, 1, n_high, 1, rows, block),
                    functools.partial(
                        lambda s, k, place: (0, source(k, place), 0, (place[1] + n_low - s) % n_low, number, k % per),
                        s,
                    ),
                )
                for s in range(n_low)
            ]
        else:
            specs = [
                pl.BlockSpec((1, n_aa, n_high, rows, block), lambda k, place: (k // per, 0, 0, 0, k % per))
            ] * n_low
        weights = pl.BlockSpec((1, block, hidden_n), lambda k, place: (0, source(k, place) * per + k % per, 0))
        return pl.pallas_call(
            functools.partial(hidden_body, steps),
            grid_spec=pltpu.PrefetchScalarGridSpec(
                num_scalar_prefetch=1,
                grid=(steps,),
                in_specs=specs + [weights, weights],
                out_specs=pl.BlockSpec((tall, hidden_n), lambda k, place: (0, 0)),
                scratch_shapes=[pltpu.VMEM((tall, hidden_n), jnp.float32)] * 2,
            ),
            out_shape=jax.ShapeDtypeStruct((tall, hidden_n), jnp.bfloat16),
            cost_estimate=pl.CostEstimate(
                flops=4 * tall * n_ba * width * hidden_n,
                transcendentals=tall * hidden_n,
                bytes_accessed=4 * n_ba * width * hidden_n + 2 * tall * n_ba * width,
            ),
            compiler_params=pltpu.CompilerParams(vmem_limit_bytes=60 * 1024 * 1024),
        )(place, *arrays, w_gate, w_up)

    def out_of(hidden, number):
        scale = lax.slice_in_dim(walked_scores if number < n_walked else scores, number * rows, (number + 1) * rows, axis=3).reshape(-1, 1)
        return pl.pallas_call(
            down_body,
            grid_spec=pltpu.PrefetchScalarGridSpec(
                num_scalar_prefetch=1,
                grid=(steps,),
                in_specs=[
                    pl.BlockSpec((tall, hidden_n), lambda k, place: (0, 0)),
                    pl.BlockSpec((1, hidden_n, block), lambda k, place: (0, 0, source(k, place) * per + k % per)),
                    pl.BlockSpec((tall, 1), lambda k, place: (0, 0)),
                ],
                out_specs=[pl.BlockSpec((1, each, block), lambda k, place: (k // per, 0, k % per))] * n_low,
            ),
            out_shape=[jax.ShapeDtypeStruct((n_ba, each, width), jnp.bfloat16)] * n_low,
            cost_estimate=pl.CostEstimate(
                flops=2 * tall * n_ba * width * hidden_n,
                transcendentals=0,
                bytes_accessed=2 * n_ba * width * hidden_n + 2 * tall * n_ba * width,
            ),
            compiler_params=pltpu.CompilerParams(vmem_limit_bytes=60 * 1024 * 1024),
        )(place, hidden, w_down, scale)

    def give_back(outs, moving):
        arrived = pair.send(outs)
        yield []
        value = total_of(outs[0], arrived).reshape(n_ba, n_aa, n_high, rows, width)
        middle = width // 256 * 128
        first, second = value[..., :middle], value[..., middle:]
        sides = feat.blocks(first, 0, False)
        walls = wide.blocks(second, 2, moving)
        got_a, got_b = feat.send(sides), wide.send(walls)
        yield [value]
        first = total_of(sides[0], got_a)
        second = total_of(walls[0], got_b)
        walls = wide.blocks(first, 1, moving)
        sides = feat.blocks(second, 0, False)
        got_a, got_b = wide.send(walls), feat.send(sides)
        yield [first, second]
        value = jnp.concatenate([total_of(walls[0], got_a), total_of(sides[0], got_b)], axis=-1)
        floors = zed.blocks(value, 0, moving)
        arrived = zed.send(floors)
        yield [value]
        yield [total_of(floors[0], arrived)]

    def walk(piece):
        value = zed.gather(piece)
        middle = width // 256 * 128
        first, second = value[..., :middle], value[..., middle:]
        first = wide.gather(first, 1)
        second = feat.gather(second)
        first = feat.gather(first)
        second = wide.gather(second, 2)
        value = jnp.concatenate([first, second], axis=-1)
        return [value] + [pair.shift(value, s) for s in range(1, n_low)]

    begin = n_walked * rows
    rest = lax.slice_in_dim(tokens, begin, tok_rows, axis=0)
    rest = lax.all_gather(rest, ("aa", "ba", "col"), axis=0, tiled=False)
    rest = [rest.reshape(n_aa, n_ba, n_high, n_low, tok_rows - begin, width)]
    sources = [
        walk(lax.slice_in_dim(tokens, c * rows, (c + 1) * rows, axis=0)) for c in range(n_walked)
    ] + [rest] * (n_calls - n_walked)

    def tie(value, others):
        return lax.optimization_barrier((value, *others))[0] if others else value

    sums, last = [], {}

    def step(number):
        last[number] = next(sums[number])
        return last[number]

    outs = []
    for number in range(n_calls):
        before = step(number - 3) if number >= 3 else []
        first, *others = sources[number]
        first = tie(first, before + outs)
        hidden = hidden_of([first] + others, max(number - n_walked, 0))
        between = [v for back in (3, 2, 1) if number >= back for v in step(number - back)]
        outs = list(out_of(tie(hidden, between), number))
        sums.append(give_back(outs, number >= n_walked))
        step(number)
    for _ in range(5):
        for number in range(n_calls):
            for last[number] in sums[number]:
                break
    return jnp.concatenate([last[c][0] for c in range(n_calls)], axis=0)


def solution(mesh):
    return jax.shard_map(
        on_device,
        mesh=mesh,
        in_specs=(
            P(("aa", "col"), "ba"),
            P(("aa", "col"), None),
            P(("aa", "col"), None),
            P(("aa", "col"), None, "ba"),
            P(("aa", "col"), None, "ba"),
            P(("aa", "col"), "ba", None),
        ),
        out_specs=P(("aa", "col"), "ba"),
        check_vma=False,
    )
```

```python
import functools

import jax
import jax.numpy as jnp
from jax import lax
from jax.experimental import pallas as pl
from jax.experimental.pallas import tpu as pltpu
from jax.sharding import PartitionSpec as P


route_scale = 2.827
n_calls = 4
n_walked = 2


class Phase:
    def __init__(self, axis, inner, outer_n, inner_n):
        self.axis, self.inner, self.outer_n, self.inner_n = axis, inner, outer_n, inner_n
        self.n = inner_n if inner else outer_n
        place = lax.axis_index(axis)
        self.me = place % inner_n if inner else place // inner_n

    def shift(self, value, step):
        pairs = []
        for out in range(self.outer_n):
            for low in range(self.inner_n):
                if self.inner:
                    to = out * self.inner_n + (low + step) % self.inner_n
                else:
                    to = (out + step) % self.outer_n * self.inner_n + low
                pairs.append((out * self.inner_n + low, to))
        return lax.ppermute(value, self.axis, pairs)

    def gather(self, value, axis=0):
        return jnp.stack([value] + [self.shift(value, s) for s in range(1, self.n)], axis=axis)

    def ordered(self, value, axis):
        return jnp.take(value, (self.me - jnp.arange(self.n)) % self.n, axis=axis)

    def blocks(self, value, axis, moving):
        if not moving:
            return [lax.index_in_dim(value, s, axis, keepdims=False) for s in range(self.n)]
        return [
            lax.dynamic_index_in_dim(value, (self.me - s) % self.n, axis, keepdims=False)
            for s in range(self.n)
        ]

    def send(self, blocks):
        return [self.shift(blocks[s], self.n - s) for s in range(1, self.n)]


def total_of(own, arrived):
    total = own.astype(jnp.float32)
    for block in arrived:
        total = total + block.astype(jnp.float32)
    return total.astype(jnp.bfloat16)


def hidden_body(steps, place, *refs):
    n_x = len(refs) - 5
    xs = refs[:n_x]
    wg, wu, out, gate, upper = refs[n_x:]
    k = pl.program_id(0)
    x = jnp.concatenate([r[...].reshape(-1, r.shape[-1]) for r in xs], axis=0)
    g = jnp.dot(x, wg[0], preferred_element_type=jnp.float32)
    u = jnp.dot(x, wu[0], preferred_element_type=jnp.float32)

    @pl.when(k == 0)
    def _():
        gate[...] = g
        upper[...] = u

    @pl.when(k > 0)
    def _():
        gate[...] += g
        upper[...] += u

    @pl.when(k == steps - 1)
    def _():
        v = gate[...]
        out[...] = (v / (1.0 + jnp.exp(-v)) * upper[...]).astype(jnp.bfloat16)


def down_body(place, hidden, wd, scale, *outs):
    y = jnp.dot(hidden[...], wd[0], preferred_element_type=jnp.float32)
    y = (y * scale[...]).astype(jnp.bfloat16)
    each = y.shape[0] // len(outs)
    for s, out in enumerate(outs):
        out[0] = y[s * each : (s + 1) * each]


def on_device(tokens, routing, gate_codes, w_gate, w_up, w_down):
    n_aa = lax.axis_size("aa")
    n_ba = lax.axis_size("ba")
    n_col = lax.axis_size("col")
    experts = n_aa * n_col
    n_low = 2 if n_col % 2 == 0 else 1
    n_high = n_col // n_low
    zed = Phase("aa", False, n_aa, 1)
    wide = Phase("col", False, n_high, n_low)
    pair = Phase("col", True, n_high, n_low)
    feat = Phase("ba", False, n_ba, 1)
    mine = lax.axis_index("aa") * n_col + lax.axis_index("col")
    tok_rows, width = tokens.shape
    hidden_n = w_gate.shape[2]
    rows = tok_rows // n_calls
    each = n_aa * n_high * rows
    tall = n_low * each
    block = 1792 if width % 1792 == 0 else width
    per = width // block
    steps = n_ba * per
    place = jnp.stack([feat.me, pair.me]).astype(jnp.int32)

    codes = gate_codes.astype(jnp.float32)
    weight = route_scale * codes / jnp.sum(codes, axis=1, keepdims=True)
    named = routing[None, :, :] == jnp.arange(experts, dtype=jnp.int32)[:, None, None]
    scores = jnp.sum(jnp.where(named, weight[None, :, :], 0.0), axis=2)
    scores = zed.gather(scores)
    scores = wide.gather(scores)
    scores = pair.gather(scores)
    own = jnp.arange(experts, dtype=jnp.int32)[:, None] == mine
    scores = jnp.sum(jnp.where(own, scores, 0.0), axis=3)
    walked_scores = jnp.swapaxes(scores, 1, 2)
    scores = wide.ordered(zed.ordered(walked_scores, 1), 2)

    def source(k, place):
        return (place[0] + n_ba - k // per) % n_ba

    def hidden_of(arrays, number):
        if len(arrays) == 1:
            arrays = arrays * n_low
            specs = [
                pl.BlockSpec(
                    (n_aa, 1, n_high, 1, rows, block),
                    functools.partial(
                        lambda s, k, place: (0, source(k, place), 0, (place[1] + n_low - s) % n_low, number, k % per),
                        s,
                    ),
                )
                for s in range(n_low)
            ]
        else:
            specs = [
                pl.BlockSpec((1, n_aa, n_high, rows, block), lambda k, place: (k // per, 0, 0, 0, k % per))
            ] * n_low
        weights = pl.BlockSpec((1, block, hidden_n), lambda k, place: (0, source(k, place) * per + k % per, 0))
        return pl.pallas_call(
            functools.partial(hidden_body, steps),
            grid_spec=pltpu.PrefetchScalarGridSpec(
                num_scalar_prefetch=1,
                grid=(steps,),
                in_specs=specs + [weights, weights],
                out_specs=pl.BlockSpec((tall, hidden_n), lambda k, place: (0, 0)),
                scratch_shapes=[pltpu.VMEM((tall, hidden_n), jnp.float32)] * 2,
            ),
            out_shape=jax.ShapeDtypeStruct((tall, hidden_n), jnp.bfloat16),
            cost_estimate=pl.CostEstimate(
                flops=4 * tall * n_ba * width * hidden_n,
                transcendentals=tall * hidden_n,
                bytes_accessed=4 * n_ba * width * hidden_n + 2 * tall * n_ba * width,
            ),
            compiler_params=pltpu.CompilerParams(vmem_limit_bytes=60 * 1024 * 1024),
        )(place, *arrays, w_gate, w_up)

    def out_of(hidden, number):
        scale = lax.slice_in_dim(walked_scores if number < n_walked else scores, number * rows, (number + 1) * rows, axis=3).reshape(-1, 1)
        return pl.pallas_call(
            down_body,
            grid_spec=pltpu.PrefetchScalarGridSpec(
                num_scalar_prefetch=1,
                grid=(steps,),
                in_specs=[
                    pl.BlockSpec((tall, hidden_n), lambda k, place: (0, 0)),
                    pl.BlockSpec((1, hidden_n, block), lambda k, place: (0, 0, source(k, place) * per + k % per)),
                    pl.BlockSpec((tall, 1), lambda k, place: (0, 0)),
                ],
                out_specs=[pl.BlockSpec((1, each, block), lambda k, place: (k // per, 0, k % per))] * n_low,
            ),
            out_shape=[jax.ShapeDtypeStruct((n_ba, each, width), jnp.bfloat16)] * n_low,
            cost_estimate=pl.CostEstimate(
                flops=2 * tall * n_ba * width * hidden_n,
                transcendentals=0,
                bytes_accessed=2 * n_ba * width * hidden_n + 2 * tall * n_ba * width,
            ),
            compiler_params=pltpu.CompilerParams(vmem_limit_bytes=60 * 1024 * 1024),
        )(place, hidden, w_down, scale)

    def give_back(outs, moving, wait, hold):
        arrived = pair.send(outs)
        yield []
        value = total_of(outs[0], arrived).reshape(n_ba, n_aa, n_high, rows, width)
        middle = width // 256 * 128
        first, second = value[..., :middle], value[..., middle:]
        sides = feat.blocks(first, 0, False)
        walls = wide.blocks(second, 2, moving)
        got_a, got_b = feat.send(sides), wide.send(walls)
        yield [value]
        if wait:
            held = lax.optimization_barrier((*got_a, *got_b, *wait))
            got_a, got_b = held[: len(got_a)], held[len(got_a) : len(got_a) + len(got_b)]
        first = total_of(sides[0], got_a)
        second = total_of(walls[0], got_b)
        walls = wide.blocks(first, 1, moving)
        sides = feat.blocks(second, 0, False)
        got_a, got_b = wide.send(walls), feat.send(sides)
        yield [first, second]
        value = jnp.concatenate([total_of(walls[0], got_a), total_of(sides[0], got_b)], axis=-1)
        floors = zed.blocks(value, 0, moving)
        arrived = zed.send(floors)
        yield [value]
        if hold:
            arrived = lax.optimization_barrier((*arrived, *hold))[: len(arrived)]
        yield [total_of(floors[0], arrived)]

    def walk(piece):
        value = zed.gather(piece)
        middle = width // 256 * 128
        first, second = value[..., :middle], value[..., middle:]
        first = wide.gather(first, 1)
        second = feat.gather(second)
        first = feat.gather(first)
        second = wide.gather(second, 2)
        value = jnp.concatenate([first, second], axis=-1)
        return [value] + [pair.shift(value, s) for s in range(1, n_low)]

    begin = n_walked * rows
    rest = lax.slice_in_dim(tokens, begin, tok_rows, axis=0)
    rest = lax.all_gather(rest, ("aa", "ba", "col"), axis=0, tiled=False)
    rest = [rest.reshape(n_aa, n_ba, n_high, n_low, tok_rows - begin, width)]
    sources = [
        walk(lax.slice_in_dim(tokens, c * rows, (c + 1) * rows, axis=0)) for c in range(n_walked)
    ] + [rest] * (n_calls - n_walked)

    def tie(value, others):
        return lax.optimization_barrier((value, *others))[0] if others else value

    sums, last, hold, waits = [], {}, [], [[] for _ in range(n_calls)]

    def step(number):
        last[number] = next(sums[number])
        return last[number]

    outs = []
    for number in range(n_calls):
        before = step(number - 3) if number >= 3 else []
        first, *others = sources[number]
        first = tie(first, before + outs)
        hidden = hidden_of([first] + others, max(number - n_walked, 0))
        between = [v for back in (3, 2, 1) if number >= back for v in step(number - back)]
        outs = list(out_of(tie(hidden, between), number))
        sums.append(give_back(outs, number >= n_walked, waits[number], hold))
        step(number)
    end = n_calls - 1
    waits[end - 1].extend(step(end))
    for number in (end - 2, end - 1, end, end - 1):
        step(number)
    hold.extend(step(end))
    for number in range(n_calls):
        for last[number] in sums[number]:
            pass
    return jnp.concatenate([last[c][0] for c in range(n_calls)], axis=0)


def solution(mesh):
    return jax.shard_map(
        on_device,
        mesh=mesh,
        in_specs=(
            P(("aa", "col"), "ba"),
            P(("aa", "col"), None),
            P(("aa", "col"), None),
            P(("aa", "col"), None, "ba"),
            P(("aa", "col"), None, "ba"),
            P(("aa", "col"), "ba", None),
        ),
        out_specs=P(("aa", "col"), "ba"),
        check_vma=False,
    )
```

```python
import functools

import jax
import jax.numpy as jnp
from jax import lax
from jax.experimental import pallas as pl
from jax.experimental.pallas import tpu as pltpu
from jax.sharding import PartitionSpec as P


route_scale = 2.827
n_calls = 4
n_walked = 2


class Phase:
    def __init__(self, axis, inner, outer_n, inner_n):
        self.axis, self.inner, self.outer_n, self.inner_n = axis, inner, outer_n, inner_n
        self.n = inner_n if inner else outer_n
        place = lax.axis_index(axis)
        self.me = place % inner_n if inner else place // inner_n

    def shift(self, value, step):
        pairs = []
        for out in range(self.outer_n):
            for low in range(self.inner_n):
                if self.inner:
                    to = out * self.inner_n + (low + step) % self.inner_n
                else:
                    to = (out + step) % self.outer_n * self.inner_n + low
                pairs.append((out * self.inner_n + low, to))
        return lax.ppermute(value, self.axis, pairs)

    def gather(self, value, axis=0):
        return jnp.stack([value] + [self.shift(value, s) for s in range(1, self.n)], axis=axis)

    def ordered(self, value, axis):
        return jnp.take(value, (self.me - jnp.arange(self.n)) % self.n, axis=axis)

    def blocks(self, value, axis, moving):
        if not moving:
            return [lax.index_in_dim(value, s, axis, keepdims=False) for s in range(self.n)]
        return [
            lax.dynamic_index_in_dim(value, (self.me - s) % self.n, axis, keepdims=False)
            for s in range(self.n)
        ]

    def send(self, blocks):
        return [self.shift(blocks[s], self.n - s) for s in range(1, self.n)]


def total_of(own, arrived):
    total = own.astype(jnp.float32)
    for block in arrived:
        total = total + block.astype(jnp.float32)
    return total.astype(jnp.bfloat16)


def hidden_body(steps, place, *refs):
    n_x = len(refs) - 5
    xs = refs[:n_x]
    wg, wu, out, gate, upper = refs[n_x:]
    k = pl.program_id(0)
    x = jnp.concatenate([r[...].reshape(-1, r.shape[-1]) for r in xs], axis=0)
    g = jnp.dot(x, wg[0], preferred_element_type=jnp.float32)
    u = jnp.dot(x, wu[0], preferred_element_type=jnp.float32)

    @pl.when(k == 0)
    def _():
        gate[...] = g
        upper[...] = u

    @pl.when(k > 0)
    def _():
        gate[...] += g
        upper[...] += u

    @pl.when(k == steps - 1)
    def _():
        v = gate[...]
        out[...] = (v / (1.0 + jnp.exp(-v)) * upper[...]).astype(jnp.bfloat16)


def down_body(place, hidden, wd, scale, out):
    y = jnp.dot(hidden[...], wd[0], preferred_element_type=jnp.float32)
    out[0] = (y * scale[...]).astype(jnp.bfloat16)


def on_device(tokens, routing, gate_codes, w_gate, w_up, w_down):
    n_aa = lax.axis_size("aa")
    n_ba = lax.axis_size("ba")
    n_col = lax.axis_size("col")
    experts = n_aa * n_col
    n_low = 2 if n_col % 2 == 0 else 1
    n_high = n_col // n_low
    zed = Phase("aa", False, n_aa, 1)
    wide = Phase("col", False, n_high, n_low)
    pair = Phase("col", True, n_high, n_low)
    feat = Phase("ba", False, n_ba, 1)
    mine = lax.axis_index("aa") * n_col + lax.axis_index("col")
    tok_rows, width = tokens.shape
    hidden_n = w_gate.shape[2]
    rows = tok_rows // n_calls
    each = n_aa * n_high * rows
    tall = n_low * each
    block = 1792 if width % 1792 == 0 else width
    per = width // block
    steps = n_ba * per
    place = jnp.stack([feat.me, pair.me]).astype(jnp.int32)

    codes = gate_codes.astype(jnp.float32)
    weight = route_scale * codes / jnp.sum(codes, axis=1, keepdims=True)
    named = routing[None, :, :] == jnp.arange(experts, dtype=jnp.int32)[:, None, None]
    scores = jnp.sum(jnp.where(named, weight[None, :, :], 0.0), axis=2)
    scores = zed.gather(scores)
    scores = wide.gather(scores)
    scores = pair.gather(scores)
    own = jnp.arange(experts, dtype=jnp.int32)[:, None] == mine
    scores = jnp.sum(jnp.where(own, scores, 0.0), axis=3)
    walked_scores = jnp.swapaxes(scores, 1, 2)
    scores = wide.ordered(zed.ordered(walked_scores, 1), 2)

    def source(k, place):
        return (place[0] + n_ba - k // per) % n_ba

    def hidden_of(arrays, number):
        if len(arrays) == 1:
            arrays = arrays * n_low
            specs = [
                pl.BlockSpec(
                    (n_aa, 1, n_high, 1, rows, block),
                    functools.partial(
                        lambda s, k, place: (0, source(k, place), 0, (place[1] + n_low - s) % n_low, number, k % per),
                        s,
                    ),
                )
                for s in range(n_low)
            ]
        else:
            specs = [
                pl.BlockSpec((1, n_aa, n_high, rows, block), lambda k, place: (k // per, 0, 0, 0, k % per))
            ] * n_low
        weights = pl.BlockSpec((1, block, hidden_n), lambda k, place: (0, source(k, place) * per + k % per, 0))
        return pl.pallas_call(
            functools.partial(hidden_body, steps),
            grid_spec=pltpu.PrefetchScalarGridSpec(
                num_scalar_prefetch=1,
                grid=(steps,),
                in_specs=specs + [weights, weights],
                out_specs=pl.BlockSpec((tall, hidden_n), lambda k, place: (0, 0)),
                scratch_shapes=[pltpu.VMEM((tall, hidden_n), jnp.float32)] * 2,
            ),
            out_shape=jax.ShapeDtypeStruct((tall, hidden_n), jnp.bfloat16),
            cost_estimate=pl.CostEstimate(
                flops=4 * tall * n_ba * width * hidden_n,
                transcendentals=tall * hidden_n,
                bytes_accessed=4 * n_ba * width * hidden_n + 2 * tall * n_ba * width,
            ),
            compiler_params=pltpu.CompilerParams(vmem_limit_bytes=60 * 1024 * 1024),
        )(place, *arrays, w_gate, w_up)

    def out_of(hidden, number, s):
        scale = lax.slice_in_dim(walked_scores if number < n_walked else scores, number * rows, (number + 1) * rows, axis=3)
        return pl.pallas_call(
            down_body,
            grid_spec=pltpu.PrefetchScalarGridSpec(
                num_scalar_prefetch=1,
                grid=(steps,),
                in_specs=[
                    pl.BlockSpec((each, hidden_n), lambda k, place: (s, 0)),
                    pl.BlockSpec((1, hidden_n, block), lambda k, place: (0, 0, source(k, place) * per + k % per)),
                    pl.BlockSpec((each, 1), lambda k, place: (s, 0)),
                ],
                out_specs=pl.BlockSpec((1, each, block), lambda k, place: (k // per, 0, k % per)),
            ),
            out_shape=jax.ShapeDtypeStruct((n_ba, each, width), jnp.bfloat16),
            cost_estimate=pl.CostEstimate(
                flops=2 * each * n_ba * width * hidden_n,
                transcendentals=0,
                bytes_accessed=2 * n_ba * width * hidden_n + 2 * each * n_ba * width,
            ),
            compiler_params=pltpu.CompilerParams(vmem_limit_bytes=60 * 1024 * 1024),
        )(place, hidden, w_down, scale.reshape(-1, 1))

    def give_back(outs, moving, wait, hold):
        arrived = pair.send(outs)
        yield []
        value = total_of(outs[0], arrived).reshape(n_ba, n_aa, n_high, rows, width)
        middle = width // 256 * 128
        first, second = value[..., :middle], value[..., middle:]
        sides = feat.blocks(first, 0, False)
        walls = wide.blocks(second, 2, moving)
        got_a, got_b = feat.send(sides), wide.send(walls)
        yield [value]
        if wait:
            held = lax.optimization_barrier((*got_a, *got_b, *wait))
            got_a, got_b = held[: len(got_a)], held[len(got_a) : len(got_a) + len(got_b)]
        first = total_of(sides[0], got_a)
        second = total_of(walls[0], got_b)
        walls = wide.blocks(first, 1, moving)
        sides = feat.blocks(second, 0, False)
        got_a, got_b = wide.send(walls), feat.send(sides)
        yield [first, second]
        value = jnp.concatenate([total_of(walls[0], got_a), total_of(sides[0], got_b)], axis=-1)
        floors = zed.blocks(value, 0, moving)
        arrived = zed.send(floors)
        yield [value]
        if hold:
            arrived = lax.optimization_barrier((*arrived, *hold))[: len(arrived)]
        yield [total_of(floors[0], arrived)]

    def walk(piece):
        value = zed.gather(piece)
        middle = width // 256 * 128
        first, second = value[..., :middle], value[..., middle:]
        first = wide.gather(first, 1)
        second = feat.gather(second)
        first = feat.gather(first)
        second = wide.gather(second, 2)
        value = jnp.concatenate([first, second], axis=-1)
        return [value] + [pair.shift(value, s) for s in range(1, n_low)]

    begin = n_walked * rows
    rest = lax.slice_in_dim(tokens, begin, tok_rows, axis=0)
    rest = lax.all_gather(rest, ("aa", "ba", "col"), axis=0, tiled=False)
    rest = [rest.reshape(n_aa, n_ba, n_high, n_low, tok_rows - begin, width)]
    sources = [
        walk(lax.slice_in_dim(tokens, c * rows, (c + 1) * rows, axis=0)) for c in range(n_walked)
    ] + [rest] * (n_calls - n_walked)

    def tie(value, others):
        return lax.optimization_barrier((value, *others))[0] if others else value

    sums, last, hold, waits = [], {}, [], [[] for _ in range(n_calls)]

    def step(number):
        last[number] = next(sums[number])
        return last[number]

    own_rows = []
    for number in range(n_calls):
        before = [v for back in (2, 1) if number >= back for v in step(number - back)]
        first, *others = sources[number]
        first = tie(first, before + own_rows)
        hidden = hidden_of([first] + others, max(number - n_walked, 0))
        between = [v for back in (2, 1) if number >= back for v in step(number - back)]
        hidden = tie(hidden, between)
        outs = [None] * n_low
        for s in range(1, n_low):
            outs[s] = out_of(hidden, number, s)
        outs[0] = out_of(tie(hidden, outs[1:]), number, 0)
        own_rows = outs[:1]
        sums.append(give_back(outs, number >= n_walked, waits[number], hold))
        step(number)
    end = n_calls - 1
    for number in (end, end - 1, end):
        step(number)
    hold.extend(step(end))
    for number in range(n_calls):
        for last[number] in sums[number]:
            pass
    return jnp.concatenate([last[c][0] for c in range(n_calls)], axis=0)


def solution(mesh):
    return jax.shard_map(
        on_device,
        mesh=mesh,
        in_specs=(
            P(("aa", "col"), "ba"),
            P(("aa", "col"), None),
            P(("aa", "col"), None),
            P(("aa", "col"), None, "ba"),
            P(("aa", "col"), None, "ba"),
            P(("aa", "col"), "ba", None),
        ),
        out_specs=P(("aa", "col"), "ba"),
        check_vma=False,
    )
```

```python
import functools

import jax
import jax.numpy as jnp
from jax import lax
from jax.experimental import pallas as pl
from jax.experimental.pallas import tpu as pltpu
from jax.sharding import PartitionSpec as P


route_scale = 2.827
n_calls = 4
n_walked = 2


class Phase:
    def __init__(self, axis, inner, outer_n, inner_n):
        self.axis, self.inner, self.outer_n, self.inner_n = axis, inner, outer_n, inner_n
        self.n = inner_n if inner else outer_n
        place = lax.axis_index(axis)
        self.me = place % inner_n if inner else place // inner_n

    def shift(self, value, step):
        pairs = []
        for out in range(self.outer_n):
            for low in range(self.inner_n):
                if self.inner:
                    to = out * self.inner_n + (low + step) % self.inner_n
                else:
                    to = (out + step) % self.outer_n * self.inner_n + low
                pairs.append((out * self.inner_n + low, to))
        return lax.ppermute(value, self.axis, pairs)

    def gather(self, value, axis=0):
        return jnp.stack([value] + [self.shift(value, s) for s in range(1, self.n)], axis=axis)

    def ordered(self, value, axis):
        return jnp.take(value, (self.me - jnp.arange(self.n)) % self.n, axis=axis)

    def blocks(self, value, axis, moving):
        if not moving:
            return [lax.index_in_dim(value, s, axis, keepdims=False) for s in range(self.n)]
        return [
            lax.dynamic_index_in_dim(value, (self.me - s) % self.n, axis, keepdims=False)
            for s in range(self.n)
        ]

    def send(self, blocks):
        return [self.shift(blocks[s], self.n - s) for s in range(1, self.n)]


def total_of(own, arrived):
    total = own.astype(jnp.float32)
    for block in arrived:
        total = total + block.astype(jnp.float32)
    return total.astype(jnp.bfloat16)


def hidden_body(steps, turns, place, *refs):
    n_x = len(refs) - 5
    xs = refs[:n_x]
    wg, wu, out, gate, upper = refs[n_x:]
    k = pl.program_id(0)
    x = jnp.concatenate([r[...].reshape(-1, r.shape[-1]) for r in xs], axis=0)
    rows = 16
    pieces = gate.shape[0] // rows

    @pl.when(k == 0)
    def _():
        @pl.loop(0, pieces)
        def _(i):
            at = pl.ds(pl.multiple_of(i * rows, rows), rows)
            gate[at, :] = jnp.zeros((rows, gate.shape[1]), jnp.float32)
            upper[at, :] = jnp.zeros((rows, gate.shape[1]), jnp.float32)

    @pl.loop(0, turns)
    def _(j):
        some = gate.shape[1] // turns
        at = pl.ds(pl.multiple_of(j * some, some), some) if turns > 1 else slice(None)
        gate[:, at] += jnp.dot(x, wg[0, :, at], preferred_element_type=jnp.float32)
        upper[:, at] += jnp.dot(x, wu[0, :, at], preferred_element_type=jnp.float32)

    @pl.when(k == steps - 1)
    def _():
        @pl.loop(0, pieces)
        def _(i):
            at = pl.ds(pl.multiple_of(i * rows, rows), rows)
            v = gate[at, :]
            out[at, :] = (v / (1.0 + jnp.exp(-v)) * upper[at, :]).astype(jnp.bfloat16)


def down_body(turns, place, hidden, wd, scale, *outs):
    @pl.loop(0, turns)
    def _(j):
        some = wd.shape[2] // turns
        at = pl.ds(pl.multiple_of(j * some, some), some) if turns > 1 else slice(None)
        y = jnp.dot(hidden[...], wd[0, :, at], preferred_element_type=jnp.float32)
        y = (y * scale[...]).astype(jnp.bfloat16)
        each = y.shape[0] // len(outs)
        for s, out in enumerate(outs):
            out[0, :, at] = y[s * each : (s + 1) * each]


def on_device(tokens, routing, gate_codes, w_gate, w_up, w_down):
    n_aa = lax.axis_size("aa")
    n_ba = lax.axis_size("ba")
    n_col = lax.axis_size("col")
    experts = n_aa * n_col
    n_low = 2 if n_col % 2 == 0 else 1
    n_high = n_col // n_low
    zed = Phase("aa", False, n_aa, 1)
    wide = Phase("col", False, n_high, n_low)
    pair = Phase("col", True, n_high, n_low)
    feat = Phase("ba", False, n_ba, 1)
    mine = lax.axis_index("aa") * n_col + lax.axis_index("col")
    tok_rows, width = tokens.shape
    hidden_n = w_gate.shape[2]
    rows = tok_rows // n_calls
    each = n_aa * n_high * rows
    tall = n_low * each
    block = 1792 if width % 1792 == 0 else width
    per = width // block
    steps = n_ba * per
    place = jnp.stack([feat.me, pair.me]).astype(jnp.int32)

    codes = gate_codes.astype(jnp.float32)
    weight = route_scale * codes / jnp.sum(codes, axis=1, keepdims=True)
    named = routing[None, :, :] == jnp.arange(experts, dtype=jnp.int32)[:, None, None]
    scores = jnp.sum(jnp.where(named, weight[None, :, :], 0.0), axis=2)
    scores = zed.gather(scores)
    scores = wide.gather(scores)
    scores = pair.gather(scores)
    own = jnp.arange(experts, dtype=jnp.int32)[:, None] == mine
    scores = jnp.sum(jnp.where(own, scores, 0.0), axis=3)
    walked_scores = jnp.swapaxes(scores, 1, 2)
    scores = wide.ordered(zed.ordered(walked_scores, 1), 2)

    def source(k, place):
        return (place[0] + n_ba - k // per) % n_ba

    def hidden_of(arrays, number, turns):
        if len(arrays) == 1:
            arrays = arrays * n_low
            specs = [
                pl.BlockSpec(
                    (n_aa, 1, n_high, 1, rows, block),
                    functools.partial(
                        lambda s, k, place: (0, source(k, place), 0, (place[1] + n_low - s) % n_low, number, k % per),
                        s,
                    ),
                )
                for s in range(n_low)
            ]
        else:
            specs = [
                pl.BlockSpec((1, n_aa, n_high, rows, block), lambda k, place: (k // per, 0, 0, 0, k % per))
            ] * n_low
        weights = pl.BlockSpec((1, block, hidden_n), lambda k, place: (0, source(k, place) * per + k % per, 0))
        return pl.pallas_call(
            functools.partial(hidden_body, steps, turns),
            grid_spec=pltpu.PrefetchScalarGridSpec(
                num_scalar_prefetch=1,
                grid=(steps,),
                in_specs=specs + [weights, weights],
                out_specs=pl.BlockSpec((tall, hidden_n), lambda k, place: (0, 0)),
                scratch_shapes=[pltpu.VMEM((tall, hidden_n), jnp.float32)] * 2,
            ),
            out_shape=jax.ShapeDtypeStruct((tall, hidden_n), jnp.bfloat16),
            cost_estimate=pl.CostEstimate(
                flops=4 * tall * n_ba * width * hidden_n,
                transcendentals=tall * hidden_n,
                bytes_accessed=4 * n_ba * width * hidden_n + 2 * tall * n_ba * width,
            ),
            compiler_params=pltpu.CompilerParams(vmem_limit_bytes=60 * 1024 * 1024),
        )(place, *arrays, w_gate, w_up)

    def out_of(hidden, number, turns):
        scale = lax.slice_in_dim(walked_scores if number < n_walked else scores, number * rows, (number + 1) * rows, axis=3)
        return pl.pallas_call(
            functools.partial(down_body, turns),
            grid_spec=pltpu.PrefetchScalarGridSpec(
                num_scalar_prefetch=1,
                grid=(steps,),
                in_specs=[
                    pl.BlockSpec((tall, hidden_n), lambda k, place: (0, 0)),
                    pl.BlockSpec((1, hidden_n, block), lambda k, place: (0, 0, source(k, place) * per + k % per)),
                    pl.BlockSpec((tall, 1), lambda k, place: (0, 0)),
                ],
                out_specs=[pl.BlockSpec((1, each, block), lambda k, place: (k // per, 0, k % per))] * n_low,
            ),
            out_shape=[jax.ShapeDtypeStruct((n_ba, each, width), jnp.bfloat16)] * n_low,
            cost_estimate=pl.CostEstimate(
                flops=2 * tall * n_ba * width * hidden_n,
                transcendentals=0,
                bytes_accessed=2 * n_ba * width * hidden_n + 2 * tall * n_ba * width,
            ),
            compiler_params=pltpu.CompilerParams(vmem_limit_bytes=60 * 1024 * 1024),
        )(place, hidden, w_down, scale.reshape(-1, 1))

    def give_back(outs, moving, wait, hold):
        arrived = pair.send(outs)
        yield []
        value = total_of(outs[0], arrived).reshape(n_ba, n_aa, n_high, rows, width)
        middle = width // 256 * 128
        first, second = value[..., :middle], value[..., middle:]
        sides = feat.blocks(first, 0, False)
        walls = wide.blocks(second, 2, moving)
        got_a, got_b = feat.send(sides), wide.send(walls)
        yield [value]
        if wait:
            held = lax.optimization_barrier((*got_a, *got_b, *wait))
            got_a, got_b = held[: len(got_a)], held[len(got_a) : len(got_a) + len(got_b)]
        first = total_of(sides[0], got_a)
        second = total_of(walls[0], got_b)
        walls = wide.blocks(first, 1, moving)
        sides = feat.blocks(second, 0, False)
        got_a, got_b = wide.send(walls), feat.send(sides)
        yield [first, second]
        value = jnp.concatenate([total_of(walls[0], got_a), total_of(sides[0], got_b)], axis=-1)
        floors = zed.blocks(value, 0, moving)
        arrived = zed.send(floors)
        yield [value]
        if hold:
            arrived = lax.optimization_barrier((*arrived, *hold))[: len(arrived)]
        yield [total_of(floors[0], arrived)]

    def walk(piece):
        value = zed.gather(piece)
        middle = width // 256 * 128
        first, second = value[..., :middle], value[..., middle:]
        first = wide.gather(first, 1)
        second = feat.gather(second)
        first = feat.gather(first)
        second = wide.gather(second, 2)
        marks.extend([first, second])
        value = jnp.concatenate([first, second], axis=-1)
        return [value] + [pair.shift(value, s) for s in range(1, n_low)]

    def tie(value, others):
        return lax.optimization_barrier((value, *others))[0] if others else value

    begin = n_walked * rows
    marks = []
    walked = [walk(lax.slice_in_dim(tokens, c * rows, (c + 1) * rows, axis=0)) for c in range(n_walked)]
    rest = tie(lax.slice_in_dim(tokens, begin, tok_rows, axis=0), marks[:2])
    rest = lax.all_gather(rest, ("aa", "ba", "col"), axis=0, tiled=False)
    rest = [rest.reshape(n_aa, n_ba, n_high, n_low, tok_rows - begin, width)]
    sources = walked + [rest] * (n_calls - n_walked)

    sums, last, hold, waits = [], {}, [], [[] for _ in range(n_calls)]

    def step(number):
        last[number] = next(sums[number])
        return last[number]

    own_rows = []
    for number in range(n_calls):
        before = [v for back in (2, 1) if number >= back for v in step(number - back)]
        turns = 2 if number < n_walked else 1
        first, *others = sources[number]
        first = tie(first, before + own_rows)
        hidden = hidden_of([first] + others, max(number - n_walked, 0), turns)
        between = [v for back in (2, 1) if number >= back for v in step(number - back)]
        outs = list(out_of(tie(hidden, between), number, turns))
        own_rows = outs[:1]
        sums.append(give_back(outs, number >= n_walked, waits[number], hold))
        step(number)
    end = n_calls - 1
    for number in (end, end - 1, end):
        step(number)
    hold.extend(step(end))
    for number in range(n_calls):
        for last[number] in sums[number]:
            pass
    return jnp.concatenate([last[c][0] for c in range(n_calls)], axis=0)


def solution(mesh):
    return jax.shard_map(
        on_device,
        mesh=mesh,
        in_specs=(
            P(("aa", "col"), "ba"),
            P(("aa", "col"), None),
            P(("aa", "col"), None),
            P(("aa", "col"), None, "ba"),
            P(("aa", "col"), None, "ba"),
            P(("aa", "col"), "ba", None),
        ),
        out_specs=P(("aa", "col"), "ba"),
        check_vma=False,
    )
```
